32 devices in a mesh: gx: 4 (over y, x), gy: 2 (over core), gz: 4 (over z).
Axes of the slice: x: 2, y: 2, z: 4, core: 2. Of those that a mesh axis runs over, the one named last changes fastest.
Arguments:
- pair_blocks: float32 [529, 1024], P(None, ('gx', 'gy', 'gz')), may hold values from -6 to 6
- basis_map: float32 [529, 64], replicated, may hold values from -0.25 to 0.25
- pair_cells: int32 [3, 1024], P(None, ('gx', 'gy', 'gz')), may hold values from 0 to 511, as said below
- pair_offsets: float32 [3, 1024], P(None, ('gx', 'gy', 'gz')), may hold values from 0 to 1
- exponent_index: int32 [1024], P(('gx', 'gy', 'gz')), may hold values from 0 to 15
- radius_index: int32 [1024], P(('gx', 'gy', 'gz')), may hold values from 0 to 4
- exponents: float32 [16], replicated, may hold values from 7 to 9
Outputs:
- density: float32 [32, 64, 512], P('gx', 'gy', 'gz')
- spectrum: float32 [2, 512, 64, 32], P(None, ('gy', 'gz'), 'gx')
The draws below stay inside these ranges and needn't reach their ends.
Inputs may be any that keep to these rules, and one draw needn't show every extreme that they name: The y of pair_cells column p lies among the 32 cells, and its z among the 128 cells, of the gy and gz index of the device that holds column p. Of the pairs that one device holds at most 16 have x in the same run of 8 cells that one gx index holds, and in every draw some such run gets exactly 16 from every device.
All inputs are finite; a program needn't handle non-finite values.
Results may differ from the reference program's by a relative error of at most 0.0003.
Values sent between devices are 32-bit elements; how exact they have to be, the bound alone decides.
A program may use at most 64 MiB of HBM per device.

```python
import math
import jax
import jax.numpy as jnp
from jax import lax

BLOCK = 23
DEG = 3
NPOLY = 64
NEXP = 16
HALO = 8
CX = 8
CY = 32
CZ = 128
PAIR_DEV = 32
CAP = 16
PAIRS = 1024
NX = 32
NY = 64
NZ = 512
N_GX = 4
N_GY = 2
N_GZ = 4


def draw_pair_cells(key, part):
    source_count = N_GX * N_GY * N_GZ
    slot_count = N_GX * CAP
    key_level, key_top, key_pick, key_perm, key_x, key_y, key_z = jax.random.split(key, 7)
    levels = jax.random.randint(key_level, (N_GX,), 0, 4)
    favourite = jax.random.randint(key_top, (), 0, N_GX)
    levels = jnp.where(jnp.arange(N_GX) == favourite, 4, levels)
    sources = jnp.arange(source_count, dtype=jnp.int32)
    slot_ids = jnp.arange(slot_count, dtype=jnp.int32)
    slot_target = slot_ids // CAP
    first_slot = slot_ids % CAP == 0
    edge_class = (slot_target[None, :] + sources[:, None]) % 4
    upper_edge = first_slot[None, :] & (edge_class == 0)
    lower_edge = first_slot[None, :] & (edge_class == 2)
    slot_levels = jnp.where(upper_edge | lower_edge, 5, levels[slot_target][None, :])
    noise = jax.random.randint(key_pick, (source_count, slot_count), 0, 65536)
    scores = (slot_levels * 65536 + noise) * slot_count + slot_ids[None, :]
    unused, chosen = lax.top_k(scores, PAIR_DEV)
    orders = jax.vmap(lambda sub_key: jax.random.permutation(sub_key, PAIR_DEV))(jax.random.split(key_perm, source_count))
    chosen = jnp.take_along_axis(chosen, orders, 1)
    targets = chosen // CAP
    chosen_upper = jnp.take_along_axis(upper_edge, chosen, 1)
    chosen_lower = jnp.take_along_axis(lower_edge, chosen, 1)
    source_y = sources // N_GZ % N_GY
    source_z = sources % N_GZ
    inner_x = jax.random.randint(key_x, (source_count, PAIR_DEV), 0, CX)
    inner_x = jnp.where(chosen_upper, CX - 1, jnp.where(chosen_lower, 0, inner_x))
    cells_x = targets * CX + inner_x
    cells_y = source_y[:, None] * CY + jax.random.randint(key_y, (source_count, PAIR_DEV), 0, CY)
    cells_z = source_z[:, None] * CZ + jax.random.randint(key_z, (source_count, PAIR_DEV), 0, CZ)
    return jnp.stack([cells_x, cells_y, cells_z]).reshape(3, source_count * PAIR_DEV).astype(jnp.int32)


def set_ends(entries, own_key, low, high):
    extent = entries.shape
    place = [jax.random.randint(jax.random.fold_in(own_key, axis), (), 0, extent[axis]) for axis in range(len(extent))]
    entries = entries.at[tuple(place)].set(low)
    longest = extent.index(max(extent))
    place[longest] = (place[longest] + 1) % extent[longest]
    return entries.at[tuple(place)].set(high)


def steps_of(stream_key, dims, cuts, low, largest):
    level = 1.0
    for position, blocks in cuts:
        steps = jax.random.uniform(jax.random.fold_in(jax.random.fold_in(stream_key, 6), position), (blocks,), jnp.float32, low / len(cuts), largest / len(cuts))
        level = level * jnp.repeat(jnp.exp(steps), dims[position] // blocks).reshape((-1,) + (1,) * (len(dims) - 1 - position))
    return level


def centred(rng, dims, scale, limit, shards=(), kind=jnp.bfloat16):
    factor_of = steps_of(rng, dims, shards, -0.22, 0.18) if shards else 1.0
    entries = jax.random.normal(rng, dims, jnp.float32) * scale * factor_of
    return jnp.minimum(jnp.maximum(entries, -limit), limit).astype(kind)


def setup_inputs(seed: int = 0) -> dict:
    seeds = jax.random.split(jax.random.key(seed), 8)
    pair_blocks = centred(seeds[0], (BLOCK * BLOCK, PAIRS), 1.0, 6.0, ((1, 32),), jnp.float32)
    basis_map = centred(seeds[1], (BLOCK * BLOCK, NPOLY), (BLOCK * BLOCK) ** -0.5, 0.25, (), jnp.float32)
    pair_cells = draw_pair_cells(jax.random.fold_in(seeds[7], 71), 0)
    pair_offsets = jnp.clip(1.0 * jax.random.uniform(seeds[3], (3, PAIRS), jnp.float32) ** steps_of(seeds[3], (3, PAIRS), ((1, 32),), -0.2, 0.2), 0.0, 1.0)
    exponent_index = set_ends(jax.random.randint(seeds[4], (PAIRS,), 0, NEXP), jax.random.fold_in(seeds[4], 1), 0, NEXP - 1).astype(jnp.int32)
    radius_index = set_ends(jax.random.randint(seeds[5], (PAIRS,), 0, HALO // 2 + 1), jax.random.fold_in(seeds[5], 1), 0, (HALO // 2 + 1) - 1).astype(jnp.int32)
    exponents = jnp.clip(jnp.exp(jax.random.uniform(seeds[6], (NEXP,), jnp.float32, math.log(7.0), math.log(9.0))), 7.0, 9.0)
    return dict(pair_blocks=pair_blocks, basis_map=basis_map, pair_cells=pair_cells, pair_offsets=pair_offsets, exponent_index=exponent_index, radius_index=radius_index, exponents=exponents)


highest = lax.Precision.HIGHEST


def pair_factors(offsets_row, exponent_values, radius_cells):
    span = jnp.arange(2 * HALO + 1, dtype=jnp.int32) - HALO
    distance = span[None, :].astype(jnp.float32) - offsets_row[:, None]
    inside = (jnp.abs(span)[None, :] <= radius_cells[:, None]).astype(jnp.float32)
    envelope = jnp.exp(-exponent_values[:, None] * distance * distance) * inside
    scaled = distance / HALO
    return jnp.stack([scaled ** degree * envelope for degree in range(DEG + 1)], 1)


def reference(pair_blocks, basis_map, pair_cells, pair_offsets, exponent_index, radius_index, exponents):
    side = DEG + 1
    pair_total = pair_blocks.shape[1]
    group_size = 64
    group_count = pair_total // group_size
    coefficients = jnp.dot(basis_map.T, pair_blocks, precision=highest)
    radius_cells = HALO - radius_index
    radius_float = radius_cells.astype(jnp.float32)
    exponent_values = exponents[exponent_index] / (radius_float * radius_float)
    span = jnp.arange(2 * HALO + 1, dtype=jnp.int32) - HALO

    def regroup(values):
        return values.reshape((group_count, group_size) + values.shape[1:])

    pieces_all = (regroup(coefficients.T.reshape(pair_total, side, side, side)),
                  regroup(pair_factors(pair_offsets[0], exponent_values, radius_cells)),
                  regroup(pair_factors(pair_offsets[1], exponent_values, radius_cells)),
                  regroup(pair_factors(pair_offsets[2], exponent_values, radius_cells)),
                  regroup(pair_cells.T))

    def add_group(density_grid, pieces):
        pair_coefs, along_x, along_y, along_z, centre_cells = pieces
        partial_z = jnp.einsum('sijk,skc->sijc', pair_coefs, along_z, precision=highest)
        partial_y = jnp.einsum('sjb,sijc->sibc', along_y, partial_z, precision=highest)
        tile_values = jnp.einsum('sia,sibc->sabc', along_x, partial_y, precision=highest)
        rows_x = (centre_cells[:, 0:1] + span[None, :]) % NX
        rows_y = (centre_cells[:, 1:2] + span[None, :]) % NY
        rows_z = (centre_cells[:, 2:3] + span[None, :]) % NZ
        density_grid = density_grid.at[rows_x[:, :, None, None], rows_y[:, None, :, None], rows_z[:, None, None, :]].add(tile_values)
        return density_grid, None

    density, unused = lax.scan(add_group, jnp.zeros((NX, NY, NZ), jnp.float32), pieces_all)
    transform = jnp.fft.fftn(jnp.transpose(density, (2, 1, 0)), norm="ortho")
    spectrum = jnp.stack([jnp.real(transform), jnp.imag(transform)]).astype(jnp.float32)
    return density, spectrum
```

```python
import functools
import math

import jax
import jax.numpy as jnp
import numpy as np
from jax import lax
from jax.experimental import pallas as pl
from jax.experimental.pallas import tpu as pltpu
from jax.sharding import PartitionSpec as P

DEG = 3
HALO = 8
CX = 8
CY = 32
CZ = 128
SIDE = DEG + 1
LANES = 128
SPAN = 24

highest = lax.Precision.HIGHEST
f32 = jnp.float32
bf16 = jnp.bfloat16


def iota_f(shape, dim):
    return lax.broadcasted_iota(jnp.int32, shape, dim).astype(f32)


def cos_sin(turns):
    r = turns - jnp.floor(turns + 0.5)
    t = r * math.pi
    t2 = t * t
    s = t * _poly(t2, [(-1) ** n / math.factorial(2 * n + 1) for n in range(7)])
    c = _poly(t2, [(-1) ** n / math.factorial(2 * n) for n in range(8)])
    return 1.0 - 2.0 * s * s, 2.0 * s * c


def _poly(x, coefs):
    out = jnp.full_like(x, coefs[-1])
    for a in reversed(coefs[:-1]):
        out = out * x + a
    return out


def wrapped(cells, centre, total):
    d = cells - centre
    d = jnp.where(d < -HALO, d + total, d)
    return jnp.where(d > total - 1 - HALO, d - total, d)


def factors(offset, within, rate, radius):
    u = offset - within
    env = jnp.exp(-rate * u * u) * (jnp.abs(offset) <= radius).astype(f32)
    s = u * (1.0 / HALO)
    out = [env]
    for _ in range(DEG):
        out.append(out[-1] * s)
    return out


def split(v):
    hi = v.astype(bf16)
    return hi, (v - hi.astype(f32)).astype(bf16)


def nt(a, b):
    return lax.dot_general(a, b, (((1,), (1,)), ((), ())), preferred_element_type=f32)


def spectral(frequency, length, centre, within, rate, radius, table):
    n = frequency.shape[0]
    offs = iota_f((SPAN, LANES), 0) - HALO
    four = jnp.concatenate(factors(offs, within, rate, radius), axis=1)
    part = jnp.dot(table, four, precision=highest, preferred_element_type=f32)
    pc, ps = cos_sin(frequency * centre * (1.0 / length))
    out = []
    for d in range(SIDE):
        a = part[:n, d * LANES : (d + 1) * LANES]
        b = part[n:, d * LANES : (d + 1) * LANES]
        out.append((a * pc + b * ps, b * pc - a * ps))
    return out


def span_table(frequency, length):
    offs = iota_f((1, SPAN), 1) - HALO
    c, s = cos_sin(frequency * offs * (1.0 / length))
    return jnp.concatenate([c, -s], axis=0)


def chunk_work(prm, sizes, place, refs, first):
    nx, ny, nz, nky, nkz = sizes
    gx, gy, gz, kz0 = place
    (h_s, hd_s, fxl_s, t_hi, t_lo, d_hi, d_lo, z_s, zd_s, ytab, ztab, acc, acc_lo, dacc, dacc_lo) = refs
    rows = lambda a: prm[a : a + 1, :]
    base = SIDE**3
    cx, cy, cz, ox, oy, oz, rate, radius = [rows(base + n) for n in range(8)]
    kyc = iota_f((nky, 1), 0) + (gx * nky).astype(f32)
    kzc = iota_f((nkz, 1), 0) + (kz0 * nkz).astype(f32)
    fy = spectral(kyc, ny, cy, oy, rate, radius, ytab[...])
    fz = spectral(kzc, nz, cz, oz, rate, radius, ztab[...])
    fx = factors(wrapped(iota_f((nx, LANES), 0), cx, float(nx)), ox, rate, radius)
    fyl = factors(
        wrapped(iota_f((CY, LANES), 0) + (gy * CY).astype(f32), cy, float(ny)), oy, rate, radius
    )
    fzl = factors(
        wrapped(iota_f((CZ, LANES), 0) + (gz * CZ).astype(f32), cz, float(nz)), oz, rate, radius
    )
    fxl = factors(
        wrapped(iota_f((CX, LANES), 0) + (gx * CX).astype(f32), cx, float(nx)), ox, rate, radius
    )
    for i in range(SIDE):
        fxl_s[i] = fxl[i]
    for k in range(SIDE):
        lanes = slice(k * LANES, (k + 1) * LANES)
        zhi, zlo = split(jnp.concatenate(fz[k], axis=0))
        z_s[: 2 * nkz, lanes] = zhi
        z_s[2 * nkz :, lanes] = zlo
        zhi, zlo = split(fzl[k])
        zd_s[:CZ, lanes] = zhi
        zd_s[CZ:, lanes] = zlo
        for i in range(SIDE):
            re = im = de = None
            for j in range(SIDE):
                c = rows((i * SIDE + j) * SIDE + k)
                re = c * fy[j][0] if re is None else re + c * fy[j][0]
                im = c * fy[j][1] if im is None else im + c * fy[j][1]
                de = c * fyl[j] if de is None else de + c * fyl[j]
            h_s[k * SIDE + i, :nky] = re
            h_s[k * SIDE + i, nky:] = im
            hd_s[k * SIDE + i] = de
    group = 4

    def mix(g, carry):
        for rr in range(group):
            r = g * group + rr
            for k in range(SIDE):
                v = None
                for i in range(SIDE):
                    w = h_s[k * SIDE + i, pl.ds(r, 1), :] * fx[i]
                    v = w if v is None else v + w
                hi, lo = split(v)
                t_hi[pl.ds(pl.multiple_of(r * nx, nx), nx), k * LANES : (k + 1) * LANES] = hi
                t_lo[pl.ds(pl.multiple_of(r * nx, nx), nx), k * LANES : (k + 1) * LANES] = lo
        return carry

    lax.fori_loop(0, 2 * nky // group, mix, 0)
    for k in range(SIDE):
        for x in range(CX):
            v = None
            for i in range(SIDE):
                w = hd_s[k * SIDE + i] * fxl_s[i, x : x + 1, :]
                v = w if v is None else v + w
            hi, lo = split(v)
            d_hi[x * CY : (x + 1) * CY, k * LANES : (k + 1) * LANES] = hi
            d_lo[x * CY : (x + 1) * CY, k * LANES : (k + 1) * LANES] = lo
    block = 256
    for b in range(2 * nky * nx // block):
        s = slice(b * block, (b + 1) * block)
        acc[s] = acc[s] + nt(t_hi[s], z_s[...])
        acc_lo[s] = acc_lo[s] + nt(t_lo[s], z_s[: 2 * nkz])
    dacc[...] = dacc[...] + nt(d_hi[...], zd_s[...])
    dacc_lo[...] = dacc_lo[...] + nt(d_lo[...], zd_s[:CZ])


def finish(sizes, acc, acc_lo, dacc, dacc_lo, xtab, dens_ref, spec_ref):
    nx, ny, nz, nky, nkz = sizes
    dens_ref[...] = dacc[:, :CZ] + dacc[:, CZ:] + dacc_lo[...]
    wide = max(nx, LANES)
    per = wide // nx
    for g in range(nky // per):

        def take(r0):
            s = slice(r0, r0 + wide)
            v = acc[s, : 2 * nkz] + acc[s, 2 * nkz :] + acc_lo[s]
            return v.T

        re = take(g * wide)
        im = take(nky * nx + g * wide)
        c_re = re[:nkz] - im[nkz:]
        c_im = re[nkz:] + im[:nkz]
        both = jnp.concatenate([c_re, c_im], axis=0)
        q = jnp.dot(both, xtab[...], precision=highest, preferred_element_type=f32)
        spec_ref[0, :, g * wide : (g + 1) * wide] = q[:nkz, :wide] + q[nkz:, wide:]
        spec_ref[1, :, g * wide : (g + 1) * wide] = q[nkz:, :wide] - q[:nkz, wide:]


def scratches(sizes):
    nx, ny, nz, nky, nkz = sizes
    m = 2 * nky * nx
    k = SIDE * LANES
    return [
        pltpu.VMEM((SIDE * SIDE, 2 * nky, LANES), f32),
        pltpu.VMEM((SIDE * SIDE, CY, LANES), f32),
        pltpu.VMEM((SIDE, CX, LANES), f32),
        pltpu.VMEM((m, k), bf16),
        pltpu.VMEM((m, k), bf16),
        pltpu.VMEM((CX * CY, k), bf16),
        pltpu.VMEM((CX * CY, k), bf16),
        pltpu.VMEM((4 * nkz, k), bf16),
        pltpu.VMEM((2 * CZ, k), bf16),
        pltpu.VMEM((2 * nky, SPAN), f32),
        pltpu.VMEM((2 * nkz, SPAN), f32),
        pltpu.VMEM((m, 4 * nkz), f32),
        pltpu.VMEM((m, 2 * nkz), f32),
        pltpu.VMEM((CX * CY, 2 * CZ), f32),
        pltpu.VMEM((CX * CY, CZ), f32),
    ]


def start_work(sizes, place, refs):
    nx, ny, nz, nky, nkz = sizes
    gx, gy, gz, kz0 = place
    ytab, ztab, acc, acc_lo, dacc, dacc_lo = refs[-6:]
    kyc = iota_f((nky, 1), 0) + (gx * nky).astype(f32)
    kzc = iota_f((nkz, 1), 0) + (kz0 * nkz).astype(f32)
    ytab[...] = span_table(kyc, ny)
    ztab[...] = span_table(kzc, nz)
    for r in (acc, acc_lo, dacc, dacc_lo):
        r[...] = jnp.zeros_like(r)


def where_am_i():
    gx, gy, gz = (lax.axis_index(a) for a in ("gx", "gy", "gz"))
    return gx, gy, gz, gy * lax.axis_size("gz") + gz


def kernel(sizes, prm_ref, xtab, dens_ref, spec_ref, *refs):
    place = where_am_i()
    start_work(sizes, place, refs)

    def step(c, carry):
        prm = prm_ref[:, pl.ds(pl.multiple_of(c * LANES, LANES), LANES)]
        chunk_work(prm, sizes, place, refs, None)
        return carry

    lax.fori_loop(0, prm_ref.shape[1] // LANES, step, 0)
    finish(sizes, *refs[-4:], xtab, dens_ref, spec_ref)


def x_table(nx, total):
    wide = max(nx, LANES)
    idx = np.arange(nx)
    angle = (idx[:, None] * idx[None, :] % nx) * (2.0 * math.pi / nx)
    eye = np.eye(wide // nx)
    scale = 1.0 / math.sqrt(total)
    return np.concatenate(
        [np.kron(eye, np.cos(angle)), np.kron(eye, np.sin(angle))], axis=1
    ).astype(np.float32) * np.float32(scale)


def shards(
    pair_blocks, basis_map, pair_cells, pair_offsets, exponent_index, radius_index, exponents
):
    n_gx, n_gy, n_gz = (lax.axis_size(a) for a in ("gx", "gy", "gz"))
    nx, ny, nz = CX * n_gx, CY * n_gy, CZ * n_gz
    sizes = (nx, ny, nz, ny // n_gx, nz // (n_gy * n_gz))
    nky, nkz = sizes[3:]
    selector = (
        exponent_index[None, :] == jnp.arange(exponents.shape[0], dtype=jnp.int32)[:, None]
    ).astype(f32)
    radius = (HALO - radius_index).astype(f32)
    rate = jnp.sum(exponents[:, None] * selector, axis=0) / (radius * radius)
    coefs = jnp.dot(basis_map.T, pair_blocks, precision=highest)
    prm = jnp.concatenate(
        [coefs, pair_cells.astype(f32), pair_offsets, rate[None], radius[None]], axis=0
    )
    prm = lax.all_gather(prm, ("gx", "gy", "gz"), axis=1, tiled=True)
    dens, spec = pl.pallas_call(
        functools.partial(kernel, sizes),
        out_shape=[
            jax.ShapeDtypeStruct((CX * CY, CZ), f32),
            jax.ShapeDtypeStruct((2, nkz, nky * nx), f32),
        ],
        in_specs=[pl.BlockSpec(memory_space=pltpu.VMEM)] * 2,
        out_specs=[pl.BlockSpec(memory_space=pltpu.VMEM)] * 2,
        scratch_shapes=scratches(sizes),
    )(prm, jnp.asarray(x_table(nx, nx * ny * nz)))
    return dens.reshape(CX, CY, CZ), spec.reshape(2, nkz, nky, nx)


def solution(mesh):
    placed = (
        P(None, ("gx", "gy", "gz")),
        P(),
        P(None, ("gx", "gy", "gz")),
        P(None, ("gx", "gy", "gz")),
        P(("gx", "gy", "gz")),
        P(("gx", "gy", "gz")),
        P(),
    )
    return jax.shard_map(
        shards,
        mesh=mesh,
        in_specs=placed,
        out_specs=(P("gx", "gy", "gz"), P(None, ("gy", "gz"), "gx", None)),
        check_vma=False,
    )
```

```python
import functools
import math

import jax
import jax.numpy as jnp
import numpy as np
from jax import lax
from jax.experimental import pallas as pl
from jax.experimental.pallas import tpu as pltpu
from jax.sharding import PartitionSpec as P

DEG = 3
HALO = 8
CX = 8
CY = 32
CZ = 128
SIDE = DEG + 1
LANES = 128
SPAN = 24

highest = lax.Precision.HIGHEST
f32 = jnp.float32
bf16 = jnp.bfloat16


def iota_f(shape, dim):
    return lax.broadcasted_iota(jnp.int32, shape, dim).astype(f32)


def cos_sin(turns):
    r = turns - jnp.floor(turns + 0.5)
    t = r * math.pi
    t2 = t * t
    s = t * _poly(t2, [(-1) ** n / math.factorial(2 * n + 1) for n in range(7)])
    c = _poly(t2, [(-1) ** n / math.factorial(2 * n) for n in range(8)])
    return 1.0 - 2.0 * s * s, 2.0 * s * c


def _poly(x, coefs):
    out = jnp.full_like(x, coefs[-1])
    for a in reversed(coefs[:-1]):
        out = out * x + a
    return out


def wrapped(cells, centre, total):
    d = cells - centre
    d = jnp.where(d < -HALO, d + total, d)
    return jnp.where(d > total - 1 - HALO, d - total, d)


def factors(offset, within, rate, radius):
    u = offset - within
    env = jnp.exp(-rate * u * u) * (jnp.abs(offset) <= radius).astype(f32)
    s = u * (1.0 / HALO)
    out = [env]
    for _ in range(DEG):
        out.append(out[-1] * s)
    return out


def split(v):
    hi = v.astype(bf16)
    return hi, (v - hi.astype(f32)).astype(bf16)


def nt(a, b):
    return lax.dot_general(a, b, (((1,), (1,)), ((), ())), preferred_element_type=f32)


def spectral(frequency, length, centre, within, rate, radius, table):
    n = frequency.shape[0]
    offs = iota_f((SPAN, LANES), 0) - HALO
    four = jnp.concatenate(factors(offs, within, rate, radius), axis=1)
    part = jnp.dot(table, four, precision=highest, preferred_element_type=f32)
    pc, ps = cos_sin(frequency * centre * (1.0 / length))
    out = []
    for d in range(SIDE):
        a = part[:n, d * LANES : (d + 1) * LANES]
        b = part[n:, d * LANES : (d + 1) * LANES]
        out.append((a * pc + b * ps, b * pc - a * ps))
    return out


def span_table(frequency, length):
    offs = iota_f((1, SPAN), 1) - HALO
    c, s = cos_sin(frequency * offs * (1.0 / length))
    return jnp.concatenate([c, -s], axis=0)


def chunk_work(prm, sizes, place, refs):
    nx, ny, nz, nky, nkz = sizes
    gx, gy, gz, kz0 = place
    (h_s, hd_s, fxl_s, t_hi, t_lo, d_hi, d_lo, z_s, zd_s, ytab, ztab, acc, acc_lo, dacc, dacc_lo) = refs
    rows = lambda a: prm[a : a + 1, :]
    base = SIDE**3
    cx, cy, cz, ox, oy, oz, rate, radius = [rows(base + n) for n in range(8)]
    kyc = iota_f((nky, 1), 0) + (gx * nky).astype(f32)
    kzc = iota_f((nkz, 1), 0) + (kz0 * nkz).astype(f32)
    fy = spectral(kyc, ny, cy, oy, rate, radius, ytab[...])
    fz = spectral(kzc, nz, cz, oz, rate, radius, ztab[...])
    fx = factors(wrapped(iota_f((nx, LANES), 0), cx, float(nx)), ox, rate, radius)
    fyl = factors(
        wrapped(iota_f((CY, LANES), 0) + (gy * CY).astype(f32), cy, float(ny)), oy, rate, radius
    )
    fzl = factors(
        wrapped(iota_f((CZ, LANES), 0) + (gz * CZ).astype(f32), cz, float(nz)), oz, rate, radius
    )
    fxl = factors(
        wrapped(iota_f((CX, LANES), 0) + (gx * CX).astype(f32), cx, float(nx)), ox, rate, radius
    )
    for i in range(SIDE):
        fxl_s[i] = fxl[i]
    for k in range(SIDE):
        lanes = slice(k * LANES, (k + 1) * LANES)
        zhi, zlo = split(jnp.concatenate(fz[k], axis=0))
        z_s[: 2 * nkz, lanes] = zhi
        z_s[2 * nkz :, lanes] = zlo
        zhi, zlo = split(fzl[k])
        zd_s[:CZ, lanes] = zhi
        zd_s[CZ:, lanes] = zlo
        for i in range(SIDE):
            re = im = de = None
            for j in range(SIDE):
                c = rows((i * SIDE + j) * SIDE + k)
                re = c * fy[j][0] if re is None else re + c * fy[j][0]
                im = c * fy[j][1] if im is None else im + c * fy[j][1]
                de = c * fyl[j] if de is None else de + c * fyl[j]
            h_s[k * SIDE + i, :nky] = re
            h_s[k * SIDE + i, nky:] = im
            hd_s[k * SIDE + i] = de
    group = 4

    def mix(g, carry):
        for rr in range(group):
            r = g * group + rr
            for k in range(SIDE):
                v = None
                for i in range(SIDE):
                    w = h_s[k * SIDE + i, pl.ds(r, 1), :] * fx[i]
                    v = w if v is None else v + w
                hi, lo = split(v)
                t_hi[pl.ds(pl.multiple_of(r * nx, nx), nx), k * LANES : (k + 1) * LANES] = hi
                t_lo[pl.ds(pl.multiple_of(r * nx, nx), nx), k * LANES : (k + 1) * LANES] = lo
        return carry

    lax.fori_loop(0, 2 * nky // group, mix, 0)
    for k in range(SIDE):
        for x in range(CX):
            v = None
            for i in range(SIDE):
                w = hd_s[k * SIDE + i] * fxl_s[i, x : x + 1, :]
                v = w if v is None else v + w
            hi, lo = split(v)
            d_hi[x * CY : (x + 1) * CY, k * LANES : (k + 1) * LANES] = hi
            d_lo[x * CY : (x + 1) * CY, k * LANES : (k + 1) * LANES] = lo
    block = 256
    for b in range(2 * nky * nx // block):
        s = slice(b * block, (b + 1) * block)
        acc[s] = acc[s] + nt(t_hi[s], z_s[...])
        acc_lo[s] = acc_lo[s] + nt(t_lo[s], z_s[: 2 * nkz])
    dacc[...] = dacc[...] + nt(d_hi[...], zd_s[...])
    dacc_lo[...] = dacc_lo[...] + nt(d_lo[...], zd_s[:CZ])


def finish(sizes, acc, acc_lo, dacc, dacc_lo, xtab, dens_ref, spec_ref):
    nx, ny, nz, nky, nkz = sizes
    dens_ref[...] = dacc[:, :CZ] + dacc[:, CZ:] + dacc_lo[...]
    wide = max(nx, LANES)
    per = wide // nx
    for g in range(nky // per):

        def take(r0):
            s = slice(r0, r0 + wide)
            v = acc[s, : 2 * nkz] + acc[s, 2 * nkz :] + acc_lo[s]
            return v.T

        re = take(g * wide)
        im = take(nky * nx + g * wide)
        c_re = re[:nkz] - im[nkz:]
        c_im = re[nkz:] + im[:nkz]
        both = jnp.concatenate([c_re, c_im], axis=0)
        q = jnp.dot(both, xtab[...], precision=highest, preferred_element_type=f32)
        spec_ref[0, :, g * wide : (g + 1) * wide] = q[:nkz, :wide] + q[nkz:, wide:]
        spec_ref[1, :, g * wide : (g + 1) * wide] = q[nkz:, :wide] - q[:nkz, wide:]


def scratches(sizes):
    nx, ny, nz, nky, nkz = sizes
    m = 2 * nky * nx
    k = SIDE * LANES
    return [
        pltpu.VMEM((SIDE * SIDE, 2 * nky, LANES), f32),
        pltpu.VMEM((SIDE * SIDE, CY, LANES), f32),
        pltpu.VMEM((SIDE, CX, LANES), f32),
        pltpu.VMEM((m, k), bf16),
        pltpu.VMEM((m, k), bf16),
        pltpu.VMEM((CX * CY, k), bf16),
        pltpu.VMEM((CX * CY, k), bf16),
        pltpu.VMEM((4 * nkz, k), bf16),
        pltpu.VMEM((2 * CZ, k), bf16),
        pltpu.VMEM((2 * nky, SPAN), f32),
        pltpu.VMEM((2 * nkz, SPAN), f32),
        pltpu.VMEM((m, 4 * nkz), f32),
        pltpu.VMEM((m, 2 * nkz), f32),
        pltpu.VMEM((CX * CY, 2 * CZ), f32),
        pltpu.VMEM((CX * CY, CZ), f32),
    ]


def start_work(sizes, place, refs):
    nx, ny, nz, nky, nkz = sizes
    gx, gy, gz, kz0 = place
    ytab, ztab, acc, acc_lo, dacc, dacc_lo = refs[-6:]
    kyc = iota_f((nky, 1), 0) + (gx * nky).astype(f32)
    kzc = iota_f((nkz, 1), 0) + (kz0 * nkz).astype(f32)
    ytab[...] = span_table(kyc, ny)
    ztab[...] = span_table(kzc, nz)
    for r in (acc, acc_lo, dacc, dacc_lo):
        r[...] = jnp.zeros_like(r)


def where_am_i():
    gx, gy, gz = (lax.axis_index(a) for a in ("gx", "gy", "gz"))
    return gx, gy, gz, gy * lax.axis_size("gz") + gz


def unpack(blocks, prm):
    owner = lax.broadcasted_iota(jnp.int32, (SPAN, LANES), 1) // (LANES // len(blocks))
    for g in range(prm.shape[0] // SPAN):
        v = None
        for d, block in enumerate(blocks):
            shift = (d - g) % len(blocks) * (LANES // len(blocks))
            w = pltpu.roll(block, shift, 1) if shift else block
            v = w if v is None else jnp.where(owner == d, w, v)
        prm[g * SPAN : (g + 1) * SPAN] = v


def kernel(sizes, counts, own_ref, xtab, dens_ref, spec_ref, prm, cols, *refs):
    refs, (send_z, recv_z, send_c, recv_c) = refs[:-4], refs[-4:]
    n_gx, n_gy, n_gz = counts
    place = where_am_i()
    gx, gy, gz = place[:3]
    n_col = n_gx * n_gy

    def along_z(r):
        return gx, gy, lax.rem(gz + n_gz - r, n_gz)

    def column(c):
        dx, dy = c // n_gy, c % n_gy
        return lax.rem(gx + n_gx - dx, n_gx), lax.rem(gy + n_gy - dy, n_gy), gz

    mesh_type = pl.DeviceIdType.MESH
    barrier = pltpu.get_barrier_semaphore()
    for r in range(1, n_gz):
        pl.semaphore_signal(barrier, inc=1, device_id=along_z(r), device_id_type=mesh_type)

    def greet(c, carry):
        pl.semaphore_signal(barrier, inc=1, device_id=column(c), device_id_type=mesh_type)
        return carry

    lax.fori_loop(1, n_col, greet, 0)
    cols[0, 0] = own_ref[...]
    start_work(sizes, place, refs)
    pl.semaphore_wait(barrier, n_gz + n_col - 2)

    def copy_z(r):
        return pltpu.make_async_remote_copy(
            src_ref=own_ref,
            dst_ref=cols.at[0, r],
            send_sem=send_z.at[r],
            recv_sem=recv_z.at[r],
            device_id=along_z(r),
            device_id_type=mesh_type,
        )

    def copy_c(c):
        return pltpu.make_async_remote_copy(
            src_ref=cols.at[0],
            dst_ref=cols.at[c],
            send_sem=send_c.at[c],
            recv_sem=recv_c.at[c],
            device_id=column(c),
            device_id_type=mesh_type,
        )

    for r in range(1, n_gz):
        copy_z(r).start()
    for r in range(1, n_gz):
        copy_z(r).wait_recv()

    def send(c, carry):
        copy_c(c).start()
        return carry

    lax.fori_loop(1, n_col, send, 0)

    def step(c, carry):
        @pl.when(c > 0)
        def _():
            copy_c(c).wait_recv()

        unpack([cols[c, r] for r in range(n_gz)], prm)
        chunk_work(prm, sizes, place, refs)
        return carry

    lax.fori_loop(0, n_col, step, 0)
    finish(sizes, *refs[-4:], xtab, dens_ref, spec_ref)
    for r in range(1, n_gz):
        copy_z(r).wait_send()

    def drain(c, carry):
        copy_c(c).wait_send()
        return carry

    lax.fori_loop(1, n_col, drain, 0)


def x_table(nx, total):
    wide = max(nx, LANES)
    idx = np.arange(nx)
    angle = (idx[:, None] * idx[None, :] % nx) * (2.0 * math.pi / nx)
    eye = np.eye(wide // nx)
    scale = 1.0 / math.sqrt(total)
    return np.concatenate(
        [np.kron(eye, np.cos(angle)), np.kron(eye, np.sin(angle))], axis=1
    ).astype(np.float32) * np.float32(scale)


def shards(
    pair_blocks, basis_map, pair_cells, pair_offsets, exponent_index, radius_index, exponents
):
    n_gx, n_gy, n_gz = (lax.axis_size(a) for a in ("gx", "gy", "gz"))
    nx, ny, nz = CX * n_gx, CY * n_gy, CZ * n_gz
    sizes = (nx, ny, nz, ny // n_gx, nz // (n_gy * n_gz))
    nky, nkz = sizes[3:]
    selector = (
        exponent_index[None, :] == jnp.arange(exponents.shape[0], dtype=jnp.int32)[:, None]
    ).astype(f32)
    radius = (HALO - radius_index).astype(f32)
    rate = jnp.sum(exponents[:, None] * selector, axis=0) / (radius * radius)
    coefs = jnp.dot(basis_map.T, pair_blocks, precision=highest)
    prm = jnp.concatenate(
        [coefs, pair_cells.astype(f32), pair_offsets, rate[None], radius[None]], axis=0
    )
    pair_dev = prm.shape[1]
    assert prm.shape[0] == 3 * SPAN and n_gz * pair_dev == LANES and n_gz >= 3
    groups = [prm[g * SPAN : (g + 1) * SPAN] for g in range(3)]
    groups.append(jnp.zeros((SPAN, LANES - 3 * pair_dev), f32))
    own = jnp.concatenate(groups, axis=1)
    n_col = n_gx * n_gy
    dens, spec = pl.pallas_call(
        functools.partial(kernel, sizes, (n_gx, n_gy, n_gz)),
        out_shape=[
            jax.ShapeDtypeStruct((CX * CY, CZ), f32),
            jax.ShapeDtypeStruct((2, nkz, nky * nx), f32),
        ],
        in_specs=[pl.BlockSpec(memory_space=pltpu.VMEM)] * 2,
        out_specs=[pl.BlockSpec(memory_space=pltpu.VMEM)] * 2,
        scratch_shapes=[
            pltpu.VMEM((3 * SPAN, LANES), f32),
            pltpu.VMEM((n_col, n_gz, SPAN, LANES), f32),
            *scratches(sizes),
            pltpu.SemaphoreType.DMA((n_gz,)),
            pltpu.SemaphoreType.DMA((n_gz,)),
            pltpu.SemaphoreType.DMA((n_col,)),
            pltpu.SemaphoreType.DMA((n_col,)),
        ],
        compiler_params=pltpu.CompilerParams(collective_id=0, has_side_effects=True),
    )(own, jnp.asarray(x_table(nx, nx * ny * nz)))
    return dens.reshape(CX, CY, CZ), spec.reshape(2, nkz, nky, nx)


def solution(mesh):
    placed = (
        P(None, ("gx", "gy", "gz")),
        P(),
        P(None, ("gx", "gy", "gz")),
        P(None, ("gx", "gy", "gz")),
        P(("gx", "gy", "gz")),
        P(("gx", "gy", "gz")),
        P(),
    )
    return jax.shard_map(
        shards,
        mesh=mesh,
        in_specs=placed,
        out_specs=(P("gx", "gy", "gz"), P(None, ("gy", "gz"), "gx", None)),
        check_vma=False,
    )
```

```python
import functools
import math

import jax
import jax.numpy as jnp
import numpy as np
from jax import lax
from jax.experimental import pallas as pl
from jax.experimental.pallas import tpu as pltpu
from jax.sharding import PartitionSpec as P

DEG = 3
HALO = 8
CX = 8
CY = 32
CZ = 128
SIDE = DEG + 1
LANES = 128
SPAN = 32
GROUP = 24

highest = lax.Precision.HIGHEST
f32 = jnp.float32
bf16 = jnp.bfloat16


def iota_f(shape, dim):
    return lax.broadcasted_iota(jnp.int32, shape, dim).astype(f32)


def cos_sin(turns):
    r = turns - jnp.floor(turns + 0.5)
    t = r * math.pi
    t2 = t * t
    s = t * _poly(t2, [(-1) ** n / math.factorial(2 * n + 1) for n in range(7)])
    c = _poly(t2, [(-1) ** n / math.factorial(2 * n) for n in range(8)])
    return 1.0 - 2.0 * s * s, 2.0 * s * c


def _poly(x, coefs):
    out = jnp.full_like(x, coefs[-1])
    for a in reversed(coefs[:-1]):
        out = out * x + a
    return out


def wrapped(cells, centre, total):
    d = cells - centre
    d = jnp.where(d < -HALO, d + total, d)
    return jnp.where(d > total - 1 - HALO, d - total, d)


def factors(offset, within, rate, radius):
    u = offset - within
    env = jnp.exp(-rate * u * u) * (jnp.abs(offset) <= radius).astype(f32)
    s = u * (1.0 / HALO)
    out = [env]
    for _ in range(DEG):
        out.append(out[-1] * s)
    return out


def split(v):
    hi = v.astype(bf16)
    return hi, (v - hi.astype(f32)).astype(bf16)


def nt(a, b):
    return lax.dot_general(a, b, (((1,), (1,)), ((), ())), preferred_element_type=f32)


def spectral(frequency, length, centre, within, rate, radius, table):
    n = frequency.shape[0]
    offs = iota_f((SPAN, LANES), 0) - HALO
    four = jnp.concatenate(factors(offs, within, rate, radius), axis=1)
    hi, lo = split(four)
    part = jnp.dot(
        table, jnp.concatenate([hi, lo, hi], axis=0), preferred_element_type=f32
    )
    pc, ps = cos_sin(frequency * centre * (1.0 / length))
    out = []
    for d in range(SIDE):
        a = part[:n, d * LANES : (d + 1) * LANES]
        b = part[n:, d * LANES : (d + 1) * LANES]
        out.append((a * pc + b * ps, b * pc - a * ps))
    return out


def span_table(frequency, length):
    offs = iota_f((1, SPAN), 1) - HALO
    c, s = cos_sin(frequency * offs * (1.0 / length))
    hi, lo = split(jnp.concatenate([c, -s], axis=0))
    return jnp.concatenate([hi, hi, lo], axis=1)


def chunk_work(prm, sizes, place, refs):
    nx, ny, nz, nky, nkz = sizes
    gx, gy, gz, kz0 = place
    (h_s, hd_s, fxl_s, t_hi, t_lo, d_hi, d_lo, z_s, zd_s, ytab, ztab, acc, dacc) = refs
    rows = lambda a: prm[a : a + 1, :]
    base = SIDE**3
    cx, cy, cz, ox, oy, oz, rate, radius = [rows(base + n) for n in range(8)]
    kyc = iota_f((nky, 1), 0) + (gx * nky).astype(f32)
    kzc = iota_f((nkz, 1), 0) + (kz0 * nkz).astype(f32)
    fy = spectral(kyc, ny, cy, oy, rate, radius, ytab[...])
    fz = spectral(kzc, nz, cz, oz, rate, radius, ztab[...])
    fx = factors(wrapped(iota_f((nx, LANES), 0), cx, float(nx)), ox, rate, radius)
    fyl = factors(
        wrapped(iota_f((CY, LANES), 0) + (gy * CY).astype(f32), cy, float(ny)), oy, rate, radius
    )
    fzl = factors(
        wrapped(iota_f((CZ, LANES), 0) + (gz * CZ).astype(f32), cz, float(nz)), oz, rate, radius
    )
    fxl = factors(
        wrapped(iota_f((CX, LANES), 0) + (gx * CX).astype(f32), cx, float(nx)), ox, rate, radius
    )
    for i in range(SIDE):
        fxl_s[i] = fxl[i]
    for k in range(SIDE):
        lanes = slice(k * LANES, (k + 1) * LANES)
        zhi, zlo = split(jnp.concatenate(fz[k], axis=0))
        z_s[: 2 * nkz, lanes] = zhi
        z_s[2 * nkz :, lanes] = zlo
        zhi, zlo = split(fzl[k])
        zd_s[:CZ, lanes] = zhi
        zd_s[CZ:, lanes] = zlo
        for i in range(SIDE):
            re = im = de = None
            for j in range(SIDE):
                c = rows((i * SIDE + j) * SIDE + k)
                re = c * fy[j][0] if re is None else re + c * fy[j][0]
                im = c * fy[j][1] if im is None else im + c * fy[j][1]
                de = c * fyl[j] if de is None else de + c * fyl[j]
            h_s[k * SIDE + i, :nky] = re
            h_s[k * SIDE + i, nky:] = im
            hd_s[k * SIDE + i] = de
    def build(r):
        for k in range(SIDE):
            v = None
            for i in range(SIDE):
                w = h_s[k * SIDE + i, r : r + 1, :] * fx[i]
                v = w if v is None else v + w
            hi, lo = split(v)
            t_hi[r * nx : (r + 1) * nx, k * LANES : (k + 1) * LANES] = hi
            t_lo[r * nx : (r + 1) * nx, k * LANES : (k + 1) * LANES] = lo

    def build_cell(x):
        for k in range(SIDE):
            v = None
            for i in range(SIDE):
                w = hd_s[k * SIDE + i] * fxl_s[i, x : x + 1, :]
                v = w if v is None else v + w
            hi, lo = split(v)
            d_hi[x * CY : (x + 1) * CY, k * LANES : (k + 1) * LANES] = hi
            d_lo[x * CY : (x + 1) * CY, k * LANES : (k + 1) * LANES] = lo

    def add(target, hi, lo, z, s, n):
        if n % LANES == 0:
            both = nt(hi[s], z[...])
            more = both[:, :n] + both[:, n:]
        else:
            more = nt(hi[s], z[:n]) + nt(hi[s], z[n:])
        target[s] = target[s] + (more + nt(lo[s], z[:n]))

    block = 256
    per = max(block // nx, 1)
    block = per * nx
    for x in range(CX):
        build_cell(x)
    late = [lambda: add(dacc, d_hi, d_lo, zd_s, slice(0, CX * CY), CZ)]
    for b in range(2 * nky // per):
        for r in range(b * per, (b + 1) * per):
            build(r)
        late.pop()()
        late.append(
            lambda b=b: add(acc, t_hi, t_lo, z_s, slice(b * block, (b + 1) * block), 2 * nkz)
        )
    late.pop()()


def finish(sizes, acc, dacc, xtab, dens_ref, spec_ref):
    nx, ny, nz, nky, nkz = sizes
    dens_ref[...] = dacc[...]
    wide = max(nx, LANES)
    per = wide // nx
    for g in range(nky // per):
        re = acc[g * wide : (g + 1) * wide]
        im = acc[nky * nx + g * wide : nky * nx + (g + 1) * wide]
        both = jnp.concatenate([re[:, :nkz] - im[:, nkz:], re[:, nkz:] + im[:, :nkz]], axis=1)
        q = jnp.dot(xtab[...], both, precision=highest, preferred_element_type=f32)
        s = slice(g * wide, (g + 1) * wide)
        spec_ref[0, s] = q[:wide, :nkz] + q[wide:, nkz:]
        spec_ref[1, s] = q[:wide, nkz:] - q[wide:, :nkz]


def scratches(sizes):
    nx, ny, nz, nky, nkz = sizes
    m = 2 * nky * nx
    k = SIDE * LANES
    return [
        pltpu.VMEM((SIDE * SIDE, 2 * nky, LANES), f32),
        pltpu.VMEM((SIDE * SIDE, CY, LANES), f32),
        pltpu.VMEM((SIDE, CX, LANES), f32),
        pltpu.VMEM((m, k), bf16),
        pltpu.VMEM((m, k), bf16),
        pltpu.VMEM((CX * CY, k), bf16),
        pltpu.VMEM((CX * CY, k), bf16),
        pltpu.VMEM((4 * nkz, k), bf16),
        pltpu.VMEM((2 * CZ, k), bf16),
        pltpu.VMEM((2 * nky, 3 * SPAN), bf16),
        pltpu.VMEM((2 * nkz, 3 * SPAN), bf16),
        pltpu.VMEM((m, 2 * nkz), f32),
        pltpu.VMEM((CX * CY, CZ), f32),
    ]


def start_work(sizes, place, refs):
    nx, ny, nz, nky, nkz = sizes
    gx, gy, gz, kz0 = place
    ytab, ztab, acc, dacc = refs[-4:]
    kyc = iota_f((nky, 1), 0) + (gx * nky).astype(f32)
    kzc = iota_f((nkz, 1), 0) + (kz0 * nkz).astype(f32)
    ytab[...] = span_table(kyc, ny)
    ztab[...] = span_table(kzc, nz)
    for r in (acc, dacc):
        r[...] = jnp.zeros_like(r)


def where_am_i():
    gx, gy, gz = (lax.axis_index(a) for a in ("gx", "gy", "gz"))
    return gx, gy, gz, gy * lax.axis_size("gz") + gz


def unpack(blocks, prm):
    owner = lax.broadcasted_iota(jnp.int32, (GROUP, LANES), 1) // (LANES // len(blocks))
    for g in range(prm.shape[0] // GROUP):
        v = None
        for d, block in enumerate(blocks):
            shift = (d - g) % len(blocks) * (LANES // len(blocks))
            w = pltpu.roll(block, shift, 1) if shift else block
            v = w if v is None else jnp.where(owner == d, w, v)
        prm[g * GROUP : (g + 1) * GROUP] = v


def kernel(sizes, counts, own_ref, xtab, dens_ref, spec_ref, prm, cols, *refs):
    refs, (send_z, recv_z, send_c, recv_c) = refs[:-4], refs[-4:]
    n_gx, n_gy, n_gz = counts
    place = where_am_i()
    gx, gy, gz = place[:3]
    n_col = n_gx * n_gy

    def along_z(r):
        return gx, gy, lax.rem(gz + n_gz - r, n_gz)

    def column(c):
        dx, dy = c // n_gy, c % n_gy
        return lax.rem(gx + n_gx - dx, n_gx), lax.rem(gy + n_gy - dy, n_gy), gz

    mesh_type = pl.DeviceIdType.MESH
    barrier = pltpu.get_barrier_semaphore()
    for r in range(1, n_gz):
        pl.semaphore_signal(barrier, inc=1, device_id=along_z(r), device_id_type=mesh_type)

    def greet(c, carry):
        pl.semaphore_signal(barrier, inc=1, device_id=column(c), device_id_type=mesh_type)
        return carry

    lax.fori_loop(1, n_col, greet, 0)
    cols[0, 0] = own_ref[...]
    start_work(sizes, place, refs)
    pl.semaphore_wait(barrier, n_gz + n_col - 2)

    def copy_z(r):
        return pltpu.make_async_remote_copy(
            src_ref=own_ref,
            dst_ref=cols.at[0, r],
            send_sem=send_z.at[r],
            recv_sem=recv_z.at[r],
            device_id=along_z(r),
            device_id_type=mesh_type,
        )

    def copy_c(c):
        return pltpu.make_async_remote_copy(
            src_ref=cols.at[0],
            dst_ref=cols.at[c],
            send_sem=send_c.at[c],
            recv_sem=recv_c.at[c],
            device_id=column(c),
            device_id_type=mesh_type,
        )

    for r in range(1, n_gz):
        copy_z(r).start()
    for r in range(1, n_gz):
        copy_z(r).wait_recv()

    def send(c, carry):
        copy_c(c).start()
        return carry

    lax.fori_loop(1, n_col, send, 0)

    def step(c, carry):
        @pl.when(c > 0)
        def _():
            copy_c(c).wait_recv()

        unpack([cols[c, r] for r in range(n_gz)], prm)
        chunk_work(prm, sizes, place, refs)
        return carry

    lax.fori_loop(0, n_col, step, 0)
    finish(sizes, *refs[-2:], xtab, dens_ref, spec_ref)
    for r in range(1, n_gz):
        copy_z(r).wait_send()

    def drain(c, carry):
        copy_c(c).wait_send()
        return carry

    lax.fori_loop(1, n_col, drain, 0)


def x_table(nx, total):
    wide = max(nx, LANES)
    idx = np.arange(nx)
    angle = (idx[:, None] * idx[None, :] % nx) * (2.0 * math.pi / nx)
    eye = np.eye(wide // nx)
    scale = 1.0 / math.sqrt(total)
    return np.concatenate(
        [np.kron(eye, np.cos(angle)), np.kron(eye, np.sin(angle))], axis=0
    ).astype(np.float32) * np.float32(scale)


def shards(
    pair_blocks, basis_map, pair_cells, pair_offsets, exponent_index, radius_index, exponents
):
    n_gx, n_gy, n_gz = (lax.axis_size(a) for a in ("gx", "gy", "gz"))
    nx, ny, nz = CX * n_gx, CY * n_gy, CZ * n_gz
    sizes = (nx, ny, nz, ny // n_gx, nz // (n_gy * n_gz))
    nky, nkz = sizes[3:]
    selector = (
        exponent_index[None, :] == jnp.arange(exponents.shape[0], dtype=jnp.int32)[:, None]
    ).astype(f32)
    radius = (HALO - radius_index).astype(f32)
    rate = jnp.sum(exponents[:, None] * selector, axis=0) / (radius * radius)
    coefs = jnp.dot(basis_map.T, pair_blocks, precision=highest)
    prm = jnp.concatenate(
        [coefs, pair_cells.astype(f32), pair_offsets, rate[None], radius[None]], axis=0
    )
    pair_dev = prm.shape[1]
    assert prm.shape[0] == 3 * GROUP and n_gz * pair_dev == LANES and n_gz >= 3
    groups = [prm[g * GROUP : (g + 1) * GROUP] for g in range(3)]
    groups.append(jnp.zeros((GROUP, LANES - 3 * pair_dev), f32))
    own = jnp.concatenate(groups, axis=1)
    n_col = n_gx * n_gy
    dens, spec = pl.pallas_call(
        functools.partial(kernel, sizes, (n_gx, n_gy, n_gz)),
        out_shape=[
            jax.ShapeDtypeStruct((CX * CY, CZ), f32),
            jax.ShapeDtypeStruct((2, nky * nx, nkz), f32),
        ],
        in_specs=[pl.BlockSpec(memory_space=pltpu.VMEM)] * 2,
        out_specs=[pl.BlockSpec(memory_space=pltpu.VMEM)] * 2,
        scratch_shapes=[
            pltpu.VMEM((3 * GROUP, LANES), f32),
            pltpu.VMEM((n_col, n_gz, GROUP, LANES), f32),
            *scratches(sizes),
            pltpu.SemaphoreType.DMA((n_gz,)),
            pltpu.SemaphoreType.DMA((n_gz,)),
            pltpu.SemaphoreType.DMA((n_col,)),
            pltpu.SemaphoreType.DMA((n_col,)),
        ],
        compiler_params=pltpu.CompilerParams(collective_id=0, has_side_effects=True),
    )(own, jnp.asarray(x_table(nx, nx * ny * nz)))
    return dens.reshape(CX, CY, CZ), spec.reshape(2, nky, nx, nkz).transpose(0, 3, 1, 2)


def solution(mesh):
    placed = (
        P(None, ("gx", "gy", "gz")),
        P(),
        P(None, ("gx", "gy", "gz")),
        P(None, ("gx", "gy", "gz")),
        P(("gx", "gy", "gz")),
        P(("gx", "gy", "gz")),
        P(),
    )
    return jax.shard_map(
        shards,
        mesh=mesh,
        in_specs=placed,
        out_specs=(P("gx", "gy", "gz"), P(None, ("gy", "gz"), "gx", None)),
        check_vma=False,
    )
```
